128 devices in a mesh: rep: 8 (over y, x_hi), tp: 16 (over x_lo, z, core).
Axes of the slice: x: 4 (x_hi: 2, x_lo: 2; x = x_hi * 2 + x_lo), y: 4, z: 4, core: 2. Of those that a mesh axis runs over, the one named last changes fastest.
Arguments:
- hidden: bfloat16 [4096, 14336], P('rep'), may hold values from -6 to 6
- ln_gain: float32 [14336], replicated, may hold values from 0.1 to 1.9
- ln_shift: float32 [14336], replicated, may hold values from -3 to 3
- qkv_weight: bfloat16 [14336, 32, 384], P(('rep', 'tp')), may hold values from -0.046875 to 0.046875
- qkv_bias: float32 [32, 384], P('tp'), may hold values from -64 to 64
- out_weight: bfloat16 [14336, 32, 128], P('tp'), may hold values from -0.375 to 0.375
- out_bias: float32 [14336], P('tp'), may hold values from -3 to 3
- slope_index: int32 [32], P('tp'), may hold values from 0 to 111
Outputs:
- attended: bfloat16 [4096, 14336], P('rep', 'tp')
The draws below stay inside these ranges and needn't reach their ends.
All inputs are finite; a program needn't handle non-finite values.
Results may differ from the reference program's by a relative error of at most 0.024.
The reference program's roundings to bfloat16 on the way count: a program that leaves them out, or rounds other values in their place, can miss the bound.
Values may be sent and summed in bfloat16 or wider, within the bound.
A program may use at most 192 MiB of HBM per device.

```python
import math
import jax
import jax.numpy as jnp
from jax import lax

D = 14336
N_SLOPES = 112
HEAD_DIM = 128
HEADS_DEV = 2
SEQ = 512
HEADS = 32
TOKENS = 4096
N_REP = 8


def draw_qkv_bias(key, part):
    base = 0.5 * jax.random.normal(key, (HEADS, 3 * HEAD_DIM), jnp.float32)
    return base


def plant(entries, rng, smallest, largest):
    place = [jax.random.randint(jax.random.fold_in(rng, axis), (), 0, length) for axis, length in enumerate(entries.shape)]
    longest = entries.shape.index(max(entries.shape))
    next_to = place[:longest] + [(place[longest] + 1) % entries.shape[longest]] + place[longest + 1:]
    return entries.at[tuple(place)].set(smallest).at[tuple(next_to)].set(largest)


def block_levels(rng, extent, cuts, low, high):
    factor_of, own = 1.0, jax.random.fold_in(rng, 6)
    for dim, blocks in cuts:
        heights = jnp.exp(jax.random.uniform(jax.random.fold_in(own, dim), (blocks,), jnp.float32, low / len(cuts), high / len(cuts)))
        factor_of = factor_of * jnp.repeat(heights, extent[dim] // blocks).reshape([-1 if axis == dim else 1 for axis in range(len(extent))])
    return factor_of


def gaussian(rng, shape, width, limit, cuts=(), held_as=jnp.bfloat16):
    result = width * jax.random.normal(rng, shape, jnp.float32)
    if cuts:
        result = result * block_levels(rng, shape, cuts, -0.22, 0.18)
    return jnp.clip(result, -limit, limit).astype(held_as)


def setup_inputs(seed: int = 0) -> dict:
    seeds = jax.random.split(jax.random.key(seed), 9)
    return {
        "hidden": gaussian(seeds[0], (TOKENS, D), 1.0, 6.0, ((0, 8),)),
        "ln_gain": jnp.clip(1.0 + 0.18 * jax.random.normal(seeds[1], (D,), jnp.float32), 0.1, 1.9),
        "ln_shift": gaussian(seeds[2], (D,), 0.5, 3.0, (), jnp.float32),
        "qkv_weight": gaussian(seeds[3], (D, HEADS, 3 * HEAD_DIM), D ** -0.5, 0.046875, ((0, 128),)),
        "qkv_bias": draw_qkv_bias(jax.random.fold_in(seeds[8], 71), 0),
        "out_weight": gaussian(seeds[5], (D, HEADS, HEAD_DIM), (HEAD_DIM * HEADS_DEV) ** -0.5, 0.375, ((0, 16),)),
        "out_bias": gaussian(seeds[6], (D,), 0.5, 3.0, ((0, 16),), jnp.float32),
        "slope_index": plant(jax.random.randint(seeds[7], (HEADS,), 0, N_SLOPES), jax.random.fold_in(seeds[7], 1), 0, N_SLOPES - 1).astype(jnp.int32),
    }


epsilon = 1e-05

def slope_values(slope_index):
    power = 1 << N_SLOPES.bit_length() - 1
    index_float = slope_index.astype(jnp.float32)
    leading = jnp.exp2(-8.0 * (index_float + 1.0) / power)
    between = jnp.exp2(-4.0 * (2.0 * (index_float - power) + 1.0) / power)
    return jnp.where(slope_index < power, leading, between)

def layer_norm(hidden, ln_gain, ln_shift):
    inputs_f32 = hidden.astype(jnp.float32)
    average = lax.optimization_barrier(jnp.mean(inputs_f32, axis=-1, keepdims=True))
    centred = inputs_f32 - average
    variance = lax.optimization_barrier(jnp.mean(centred * centred, axis=-1, keepdims=True))
    return (centred * lax.rsqrt(variance + epsilon) * ln_gain + ln_shift).astype(jnp.bfloat16)

def attend(qkv_heads, slopes):
    seq_rows = qkv_heads.shape[0]
    head_count = qkv_heads.shape[1]
    head_size = qkv_heads.shape[2] // 3
    query = qkv_heads[:, :, :head_size].astype(jnp.float32)
    keys = qkv_heads[:, :, head_size:2 * head_size].astype(jnp.float32)
    values = qkv_heads[:, :, 2 * head_size:].astype(jnp.float32)
    scores = jnp.einsum('sha,tha->hst', query, keys) / math.sqrt(head_size)
    position = jnp.arange(seq_rows, dtype=jnp.int32)
    distance = (position[:, None] - position[None, :]).astype(jnp.float32)
    scores = scores - slopes[:, None, None] * distance
    scores = jnp.where(distance >= 0.0, scores, -1e+30)
    highest = lax.optimization_barrier(jnp.max(scores, axis=-1, keepdims=True))
    powered = jnp.exp(scores - highest)
    attention = (powered / lax.optimization_barrier(jnp.sum(powered, axis=-1, keepdims=True))).astype(jnp.bfloat16)
    context = jnp.einsum('hst,tha->sha', attention.astype(jnp.float32), values).astype(jnp.bfloat16)
    return context.reshape(seq_rows, head_count * head_size)

def reference(hidden, ln_gain, ln_shift, qkv_weight, qkv_bias, out_weight, out_bias, slope_index):
    normed = layer_norm(hidden, ln_gain, ln_shift)
    projected = jnp.dot(normed, qkv_weight.reshape(D, HEADS * 3 * HEAD_DIM), preferred_element_type=jnp.float32)
    qkv = (projected.reshape(TOKENS, HEADS, 3 * HEAD_DIM) + qkv_bias).astype(jnp.bfloat16)
    slopes = slope_values(slope_index)
    context = jnp.concatenate([attend(qkv[prompt * SEQ:(prompt + 1) * SEQ], slopes) for prompt in range(N_REP)], axis=0)
    out_matrix = out_weight.reshape(D, HEADS * HEAD_DIM)
    group_width = HEADS_DEV * HEAD_DIM
    running = jnp.zeros((TOKENS, D), jnp.float32)
    for group in range(HEADS // HEADS_DEV):
        context_part = context[:, group * group_width:(group + 1) * group_width]
        weight_part = out_matrix[:, group * group_width:(group + 1) * group_width]
        partial_value = lax.dot_general(context_part, weight_part, (((1,), (1,)), ((), ())), preferred_element_type=jnp.float32).astype(jnp.bfloat16)
        partial_value = lax.optimization_barrier(partial_value)
        running = running + partial_value.astype(jnp.float32)
    return (running + out_bias).astype(jnp.bfloat16)
```

```python
import functools
import math

import jax
import jax.numpy as jnp
from jax import lax
from jax.experimental import pallas as pl
from jax.experimental.pallas import tpu as pltpu
from jax.sharding import PartitionSpec as P

N_SLOPES = 112
epsilon = 1e-05
MESH = pl.DeviceIdType.MESH
BF = jnp.bfloat16
F32 = jnp.float32


def slope_values(slope_index):
    power = 1 << N_SLOPES.bit_length() - 1
    index_float = slope_index.astype(jnp.float32)
    leading = jnp.exp2(-8.0 * (index_float + 1.0) / power)
    between = jnp.exp2(-4.0 * (2.0 * (index_float - power) + 1.0) / power)
    return jnp.where(slope_index < power, leading, between)


def my_coords():
    r = lax.axis_index("rep")
    t = lax.axis_index("tp")
    y = r // 2
    x = (r % 2) * 2 + t // 8
    z = (t // 2) % 4
    c = t % 2
    return x, y, z, c


def dev(x, y, z, c):
    return (y * 2 + x // 2, (x % 2) * 8 + z * 2 + c)


ROWS = 64
KB = 3584
WR = 112
HW = 384
W_ORDER = (1, 2, 6, 3, 7, 4, 5)
J_ORDER = (0, 1, 3, 2)


def exchange_kernel(
    wt, hid, gain, shift, bias, out,
    hbuf, nrm, act, wbuf, stg, pst, prx, own,
    hs, wl, zs, zr, xs, xr, ys, yr, as_, ar, ds_, dr, ps, pr,
):
    x, y, z, c = my_coords()
    d_model = gain.shape[1]
    xl = x % 2

    bar = pltpu.get_barrier_semaphore()
    partners = []
    for k in range(1, 8):
        partners.append(dev(x, y, (z + k // 2) % 4, (c + k % 2) % 2))
    for d in range(1, 4):
        partners.append(dev((x + d) % 4, y, z, c))
        partners.append(dev(x, (y + d) % 4, z, c))
    for p in partners:
        pl.semaphore_signal(bar, inc=1, device_id=p, device_id_type=MESH)

    def row_of(p, half, cc):
        return pl.multiple_of(p * 256 + half * 128 + cc * 64, 64)

    half = [(z + p) % 2 for p in range(2)]
    loads = []
    for p in range(2):
        cp = pltpu.make_async_copy(
            hid.at[pl.ds(row_of(p, half[p], c), ROWS), :], hbuf.at[p], hs.at[p])
        cp.start()
        loads.append(cp)

    def slot(xx, k):
        s = ((z + 4 - k // 2) % 4) * 2 + (c + k % 2) % 2
        return pl.multiple_of((xx * 8 + s) * WR, 16)

    tp_own = xl * 8 + z * 2 + c
    tp_oth = (1 - xl) * 8 + z * 2 + c
    wloads = []
    for h in range(2):
        a = pltpu.make_async_copy(
            wt.at[tp_own, h], wbuf.at[h, pl.ds(slot(x, 0), WR), :], wl.at[h, 0])
        b = pltpu.make_async_copy(wt.at[tp_oth, h], stg.at[h, 0], wl.at[h, 1])
        a.start()
        b.start()
        wloads.append((a, b))

    pl.semaphore_wait(bar, len(partners))

    def rcopy(src, dst, ss, rs, to):
        return pltpu.make_async_remote_copy(
            src_ref=src, dst_ref=dst, send_sem=ss, recv_sem=rs, device_id=to, device_id_type=MESH)

    sent = []

    def z_copies(h, k):
        zz, cc = (z + k // 2) % 4, (c + k % 2) % 2
        to = dev(x, y, zz, cc)
        a = rcopy(wt.at[xl * 8 + zz * 2 + cc, h],
                  wbuf.at[h, pl.ds(slot(x, 0), WR), :], zs.at[h, k, 0], zr.at[h, k, 0], to)
        b = rcopy(wt.at[(1 - xl) * 8 + zz * 2 + cc, h],
                  stg.at[h, k], zs.at[h, k, 1], zr.at[h, k, 1], to)
        return a, b

    def x_forward(h, k):
        rows = pl.ds(slot(x, k), WR)
        for d, src in ((1, stg.at[h, k]), (3, stg.at[h, k]), (2, wbuf.at[h, rows, :])):
            cp = rcopy(src, wbuf.at[h, rows, :], xs.at[h, d - 1, k], xr.at[h, d - 1, k],
                       dev((x + d) % 4, y, z, c))
            cp.start()
            sent.append(cp)

    for h in range(2):
        for k in W_ORDER:
            for cp in z_copies(h, k):
                cp.start()
                sent.append(cp)
        for cp in wloads[h]:
            cp.wait()
        x_forward(h, 0)

    step = 512
    nblk = KB // step

    def layer_norm(p):
        def body(rb, carry):
            rows = pl.ds(pl.multiple_of(rb * 16, 16), 16)
            acc = jnp.zeros((16, step), F32)
            for i in range(d_model // step):
                acc = acc + hbuf[p, rows, i * step:(i + 1) * step].astype(F32)
            mean = jnp.sum(acc, axis=1, keepdims=True) / d_model
            acc = jnp.zeros((16, step), F32)
            for i in range(d_model // step):
                dlt = hbuf[p, rows, i * step:(i + 1) * step].astype(F32) - mean
                acc = acc + dlt * dlt
            var = jnp.sum(acc, axis=1, keepdims=True) / d_model
            rstd = lax.rsqrt(var + epsilon)
            for i in range(d_model // step):
                cols = slice(i * step, (i + 1) * step)
                dlt = hbuf[p, rows, cols].astype(F32) - mean
                val = dlt * rstd * gain[:, cols] + shift[:, cols]
                o = (i % nblk) * step
                nrm[p, i // nblk, rows, o:o + step] = val.astype(BF)
            return carry

        lax.fori_loop(0, ROWS // 16, body, 0)

    def act_rows(j, p, hf, cc):
        return act.at[j, pl.ds(row_of(p, hf, cc), ROWS), :]

    def y_copy(p, d):
        return rcopy(nrm.at[p, (y + d) % 4], act_rows(4 - d, p, half[p], c),
                     ys.at[p, d - 1], yr.at[p, 4 - d - 1], dev(x, (y + d) % 4, z, c))

    def z_partner(p):
        return (z + 5 - 2 * ((z + p) % 2)) % 4

    def a_copy(j, p):
        ref = act_rows(j, p, half[p], c)
        return rcopy(ref, ref, as_.at[j, p], ar.at[j, p], dev(x, y, z_partner(p), c))

    def d_copy(j, p, lvl):
        hf = half[p] if lvl == 0 else 1 - half[p]
        ref = act_rows(j, p, hf, c)
        return rcopy(ref, ref, ds_.at[j, p, lvl], dr.at[j, p, lvl], dev(x, y, z, 1 - c))

    def start(cp):
        cp.start()
        sent.append(cp)

    for p in range(2):
        loads[p].wait()
        layer_norm(p)
        for d in (1, 3, 2):
            start(y_copy(p, d))
        rows = pl.ds(row_of(p, half[p], c), ROWS)
        act[0, rows, :] = nrm[p, y]
        start(a_copy(0, p))
        start(d_copy(0, p, 0))

    def recv(dst, rs, like):
        rcopy(dst, dst, ps.at[0, 0], rs, like).wait_recv()

    other = dev(x, y, z, 1 - c)

    def w_arrive(h, k):
        recv(wbuf.at[h, pl.ds(slot(x, k), WR), :], zr.at[h, k, 0], other)
        recv(stg.at[h, k], zr.at[h, k, 1], other)
        x_forward(h, k)

    def y_arrive(j, p):
        recv(act_rows(j, p, half[p], c), yr.at[p, j - 1], other)
        start(a_copy(j, p))
        start(d_copy(j, p, 0))

    def a_arrive(j, p):
        recv(act_rows(j, p, 1 - half[p], c), ar.at[j, p], other)
        start(d_copy(j, p, 1))

    def d_arrive(j):
        for p in range(2):
            for lvl in range(2):
                hf = half[p] if lvl == 0 else 1 - half[p]
                recv(act_rows(j, p, hf, 1 - c), dr.at[j, p, lvl], other)

    def w_ready(h):
        for k in range(8):
            for d in range(1, 4):
                recv(wbuf.at[h, pl.ds(slot((x + 4 - d) % 4, k), WR), :], xr.at[h, d - 1, k], other)

    def tile(h, j):
        def body(i, carry):
            rows = pl.ds(pl.multiple_of(i * 256, 256), 256)
            part = jnp.dot(act[j, rows, :], wbuf[h], preferred_element_type=F32)
            if j == 0:
                own[h, rows, :] = part
            else:
                pst[h, j - 1, rows, :] = part.astype(BF)
            return carry

        lax.fori_loop(0, 2, body, 0)
        if j > 0:
            start(rcopy(pst.at[h, j - 1], prx.at[h, 4 - j - 1], ps.at[h, j - 1], pr.at[h, 4 - j - 1],
                        dev(x, (y + j) % 4, z, c)))

    def finish(h):
        for j in range(1, 4):
            recv(prx.at[h, j - 1], pr.at[h, j - 1], other)
        total = own[h] + bias[h:h + 1, :]
        for j in range(3):
            total = total + prx[h, j].astype(F32)
        out[h] = total.astype(BF)

    for k in W_ORDER:
        w_arrive(0, k)
    y_arrive(1, 0)
    y_arrive(3, 0)
    for k in W_ORDER[:4]:
        w_arrive(1, k)
    y_arrive(1, 1)
    y_arrive(3, 1)
    for k in W_ORDER[4:]:
        w_arrive(1, k)
    for p in range(2):
        a_arrive(0, p)
    y_arrive(2, 0)
    w_ready(0)
    d_arrive(0)
    tile(0, 0)
    y_arrive(2, 1)
    for p in range(2):
        a_arrive(1, p)
        a_arrive(3, p)
    for j in (1, 3):
        d_arrive(j)
        tile(0, j)
    for p in range(2):
        a_arrive(2, p)
    d_arrive(2)
    tile(0, 2)
    w_ready(1)
    for j in (1, 3, 2, 0):
        tile(1, j)
    finish(0)
    finish(1)
    for cp in sent:
        cp.wait_send()


def exchange(wt, hidden, gain, shift, bias):
    d_model = hidden.shape[1]
    dma = pltpu.SemaphoreType.DMA
    anyspec = pl.BlockSpec(memory_space=pl.ANY)
    vm = pl.BlockSpec(memory_space=pltpu.VMEM)
    return pl.pallas_call(
        exchange_kernel,
        out_shape=jax.ShapeDtypeStruct((2, 512, HW), BF),
        in_specs=[anyspec, anyspec, vm, vm, vm],
        out_specs=vm,
        scratch_shapes=[
            pltpu.VMEM((2, ROWS, d_model), BF),
            pltpu.VMEM((2, 4, ROWS, KB), BF),
            pltpu.VMEM((4, 512, KB), BF),
            pltpu.VMEM((2, KB, HW), BF),
            pltpu.VMEM((2, 8, WR, HW), BF),
            pltpu.VMEM((2, 3, 512, HW), BF),
            pltpu.VMEM((2, 3, 512, HW), BF),
            pltpu.VMEM((2, 512, HW), F32),
            dma((2,)), dma((2, 2)),
            dma((2, 8, 2)), dma((2, 8, 2)),
            dma((2, 3, 8)), dma((2, 3, 8)),
            dma((2, 3)), dma((2, 3)),
            dma((4, 2)), dma((4, 2)),
            dma((4, 2, 2)), dma((4, 2, 2)),
            dma((2, 3)), dma((2, 3)),
        ],
        compiler_params=pltpu.CompilerParams(
            collective_id=0, has_side_effects=True, vmem_limit_bytes=60 * 1024 * 1024),
        name="exchange_qkv",
    )(wt, hidden, gain, shift, bias)


def shards(hidden, ln_gain, ln_shift, qkv_weight, qkv_bias, out_weight, out_bias, slope_index):
    seq_rows = hidden.shape[0]
    heads_here = qkv_bias.shape[0]
    head_size = qkv_bias.shape[1] // 3
    wt = jnp.transpose(qkv_weight, (1, 0, 2)).reshape(16, 2, qkv_weight.shape[0], HW)
    qkv = exchange(wt, hidden, ln_gain.reshape(1, -1), ln_shift.reshape(1, -1), qkv_bias)
    query = qkv[:, :, :head_size]
    keys = qkv[:, :, head_size : 2 * head_size]
    values = qkv[:, :, 2 * head_size :]
    slopes = slope_values(slope_index)
    scores = jnp.einsum(
        "hsa,hta->hst", query, keys, preferred_element_type=jnp.float32
    ) / math.sqrt(head_size)
    position = lax.iota(jnp.int32, seq_rows)
    distance = (position[:, None] - position[None, :]).astype(jnp.float32)
    scores = scores - slopes[:, None, None] * distance
    scores = jnp.where(distance >= 0.0, scores, -1e30)
    highest = jnp.max(scores, axis=-1, keepdims=True)
    powered = jnp.exp(scores - highest)
    attention = (powered / jnp.sum(powered, axis=-1, keepdims=True)).astype(jnp.bfloat16)
    context = jnp.einsum(
        "hst,hta->sha", attention, values, preferred_element_type=jnp.float32
    ).astype(jnp.bfloat16)
    context = context.reshape(seq_rows, heads_here * head_size)
    everything = lax.all_gather(context, "tp", axis=1, tiled=True)
    out_matrix = out_weight.reshape(out_weight.shape[0], -1)
    result = jnp.einsum("sk,dk->sd", everything, out_matrix, preferred_element_type=jnp.float32)
    result = result + out_bias
    return result.astype(jnp.bfloat16)


def solution(mesh):
    return jax.shard_map(
        shards,
        mesh=mesh,
        in_specs=(
            P("rep", None),
            P(),
            P(),
            P(("rep", "tp"), None, None),
            P("tp", None),
            P("tp", None, None),
            P("tp"),
            P("tp"),
        ),
        out_specs=P("rep", "tp"),
        check_vma=False,
    )
```

```python
import math

import jax
import jax.numpy as jnp
from jax import lax
from jax.experimental import pallas as pl
from jax.experimental.pallas import tpu as pltpu
from jax.sharding import PartitionSpec as P

N_SLOPES = 112
epsilon = 1e-05
MESH = pl.DeviceIdType.MESH
BF = jnp.bfloat16
F32 = jnp.float32

SEQ = 512
ROWS = 64
KB = 3584
WR = 112
GW = 256
HD = 128
OC = 128
W_ORDER = (1, 2, 6, 3, 7, 4, 5)


def slope_values(slope_index):
    power = 1 << N_SLOPES.bit_length() - 1
    index_float = slope_index.astype(jnp.float32)
    leading = jnp.exp2(-8.0 * (index_float + 1.0) / power)
    between = jnp.exp2(-4.0 * (2.0 * (index_float - power) + 1.0) / power)
    return jnp.where(slope_index < power, leading, between)


def dev(x, y, z, c):
    return (y * 2 + x // 2, (x % 2) * 8 + z * 2 + c)


def kernel(
    wq, hid, gain, shift, bias, ow, obias, slope_index, out,
    wsrc, wtv, hbuf, nrm, act, wbuf, stg, pst, prx, qkvs, owc, owr, cbuf, acc,
    wl, hs, ol, zs, zr, xs, xr, ys, yr, as_, ar, ds_, dr, ps, pr, cs, cr, fs, fr,
):
    r = lax.axis_index("rep")
    t = lax.axis_index("tp")
    y = r // 2
    xl = t // 8
    x = (r % 2) * 2 + xl
    z = (t // 2) % 4
    c = t % 2
    x_in = (x // 2) * 2 + (1 - xl)
    d_model = 4 * KB
    other = dev(x, y, z, 1 - c)

    bar = pltpu.get_barrier_semaphore()
    partners = []
    for k in range(1, 8):
        partners.append(dev(x, y, (z + k // 2) % 4, (c + k % 2) % 2))
    for d in range(1, 4):
        partners.append(dev((x + d) % 4, y, z, c))
        partners.append(dev(x, (y + d) % 4, z, c))
        partners.append(dev(x_in, y, (z + d) % 4, c))
    for p in partners:
        pl.semaphore_signal(bar, inc=1, device_id=p, device_id_type=MESH)

    def half(p):
        return (z + p) % 2

    def row_of(p, hf, cc):
        return pl.multiple_of(p * 256 + hf * 128 + cc * 64, 64)

    wload = pltpu.make_async_copy(wq, wsrc, wl.at[0])
    wload.start()

    def h_load(p, hf, lvl, b):
        return pltpu.make_async_copy(
            hid.at[pl.ds(row_of(p, hf, c), ROWS), pl.ds(b * KB, KB)], hbuf.at[p, b], hs.at[p, lvl, b])

    for p in range(2):
        for b in range(4):
            h_load(p, half(p), 0, b).start()

    def o_load(i):
        return pltpu.make_async_copy(ow.at[pl.ds(i * OC, OC)], owc.at[i % 2], ol.at[i])

    def relay_out(i):
        o_load(i).wait()

        def body(b, carry):
            rows = pl.ds(pl.multiple_of(b * 16, 16), 16)
            dst = pl.ds(pl.multiple_of(i * OC + b * 16, 16), 16)
            turned = jnp.swapaxes(owc[i % 2, rows], 0, 1)
            for h in range(32):
                owr[h % 2, dst, (h // 2) * HD:(h // 2 + 1) * HD] = turned[h]
            return carry

        lax.fori_loop(0, OC // 16, body, 0)
        if i + 2 < 7:
            o_load(i + 2).start()

    def relay_weight(col):
        def body(b, carry):
            rows = pl.ds(pl.multiple_of(b * 16, 16), 16)
            turned = jnp.swapaxes(wsrc[rows, :, col * HD:(col + 1) * HD], 0, 1)
            for h in range(32):
                blk = (h % 2) * 3 + col
                wtv[blk // 2, h // 2, rows, (blk % 2) * HD:(blk % 2 + 1) * HD] = turned[h]
            return carry

        lax.fori_loop(0, WR // 16, body, 0)

    wload.wait()
    relay_weight(0)
    relay_weight(1)
    pl.semaphore_wait(bar, len(partners))

    def rcopy(src, dst, ss, rs, to):
        return pltpu.make_async_remote_copy(
            src_ref=src, dst_ref=dst, send_sem=ss, recv_sem=rs, device_id=to, device_id_type=MESH)

    def recv(dst, rs):
        rcopy(dst, dst, zs.at[0, 0, 0], rs, other).wait_recv()

    def slot(xx, k):
        s = ((z + 4 - k // 2) % 4) * 2 + (c + k % 2) % 2
        return pl.ds(pl.multiple_of((xx * 8 + s) * WR, 16), WR)

    tp_own = xl * 8 + z * 2 + c
    tp_oth = (1 - xl) * 8 + z * 2 + c

    def z_copies(g, k):
        zz, cc = (z + k // 2) % 4, (c + k % 2) % 2
        to = dev(x, y, zz, cc)
        return (
            rcopy(wtv.at[g, xl * 8 + zz * 2 + cc], wbuf.at[g, slot(x, 0), :],
                  zs.at[g, k, 0], zr.at[g, k, 0], to),
            rcopy(wtv.at[g, (1 - xl) * 8 + zz * 2 + cc], stg.at[g, k],
                  zs.at[g, k, 1], zr.at[g, k, 1], to),
        )

    def x_copies(g, k):
        rows = slot(x, k)
        side = wtv.at[g, tp_oth] if k == 0 else stg.at[g, k]
        across = wtv.at[g, tp_own] if k == 0 else wbuf.at[g, rows, :]
        return [
            rcopy(src, wbuf.at[g, rows, :], xs.at[g, d, k], xr.at[g, d, k],
                  dev((x + d) % 4, y, z, c))
            for d, src in ((1, side), (3, side), (2, across))
        ]

    def start(copies):
        for cp in copies:
            cp.start()

    def send_weights(g):
        for k in W_ORDER:
            start(z_copies(g, k))
        start(x_copies(g, 0))
        wbuf[g, slot(x, 0), :] = wtv[g, tp_own]

    def w_arrive(g, k):
        recv(wbuf.at[g, slot(x, k), :], zr.at[g, k, 0])
        recv(stg.at[g, k], zr.at[g, k, 1])
        start(x_copies(g, k))

    def w_ready(g):
        for k in range(8):
            for d in range(1, 4):
                recv(wbuf.at[g, slot((x + 4 - d) % 4, k), :], xr.at[g, d, k])

    step = 512
    nblk = KB // step

    def stats(p, rows):
        total = jnp.zeros((16, step), F32)
        for i in range(4 * nblk):
            o = (i % nblk) * step
            total = total + hbuf[p, i // nblk, rows, o:o + step].astype(F32)
        mean = jnp.sum(total, axis=1, keepdims=True) / d_model
        total = jnp.zeros((16, step), F32)
        for i in range(4 * nblk):
            o = (i % nblk) * step
            centred = hbuf[p, i // nblk, rows, o:o + step].astype(F32) - mean
            total = total + centred * centred
        var = jnp.sum(total, axis=1, keepdims=True) / d_model
        return mean, lax.rsqrt(var + epsilon)

    def act_rows(j, p, hf, cc):
        return act.at[j, pl.ds(row_of(p, hf, cc), ROWS), :]

    def y_copy(p, d):
        return rcopy(nrm.at[p, (y + d) % 4], act_rows(4 - d, p, half(p), c),
                     ys.at[p, d], yr.at[p, 4 - d], dev(x, (y + d) % 4, z, c))

    def a_copy(j, p):
        ref = act_rows(j, p, half(p), c)
        to = dev(x, y, (z + 5 - 2 * half(p)) % 4, c)
        return rcopy(ref, ref, as_.at[j, p], ar.at[j, p], to)

    def d_copy(j, p, lvl):
        hf = half(p) if lvl == 0 else 1 - half(p)
        ref = act_rows(j, p, hf, c)
        return rcopy(ref, ref, ds_.at[j, p, lvl], dr.at[j, p, lvl], other)

    def norm_share(p, carry):
        for b in range(4):
            h_load(p, half(p), 0, b).wait()

        def body(rb, inner):
            rows = pl.ds(pl.multiple_of(rb * 16, 16), 16)
            mean, rstd = stats(p, rows)
            for i in range(4 * nblk):
                o = (i % nblk) * step
                centred = hbuf[p, i // nblk, rows, o:o + step].astype(F32) - mean
                val = centred * rstd * gain[i // nblk, :, o:o + step] + shift[i // nblk, :, o:o + step]
                nrm[p, i // nblk, rows, o:o + step] = val.astype(BF)
            return inner

        lax.fori_loop(0, ROWS // 16, body, 0)
        for b in range(4):
            h_load(p, 1 - half(p), 1, b).start()
        start([y_copy(p, d) for d in (1, 3, 2)])
        act[0, pl.ds(row_of(p, half(p), c), ROWS), :] = nrm[p, y]
        d_copy(0, p, 0).start()
        return carry

    def norm_own(p, carry):
        for b in range(4):
            h_load(p, 1 - half(p), 1, b).wait()

        def body(rb, inner):
            rows = pl.ds(pl.multiple_of(rb * 16, 16), 16)
            mean, rstd = stats(p, rows)
            dst = pl.ds(pl.multiple_of(row_of(p, 1 - half(p), c) + rb * 16, 16), 16)
            for i in range(nblk):
                cols = slice(i * step, (i + 1) * step)
                centred = hbuf[p, y, rows, cols].astype(F32) - mean
                val = centred * rstd * gain[y, :, cols] + shift[y, :, cols]
                act[0, dst, cols] = val.astype(BF)
            return inner

        lax.fori_loop(0, ROWS // 16, body, 0)
        d_copy(0, p, 1).start()
        return carry

    def y_arrive(j, p):
        recv(act_rows(j, p, half(p), c), yr.at[p, j])
        start([a_copy(j, p), d_copy(j, p, 0)])

    def a_arrive(j, p):
        recv(act_rows(j, p, 1 - half(p), c), ar.at[j, p])
        d_copy(j, p, 1).start()

    def d_arrive(j):
        for p in range(2):
            for lvl in range(2):
                hf = half(p) if lvl == 0 else 1 - half(p)
                recv(act_rows(j, p, hf, 1 - c), dr.at[j, p, lvl])

    def p_copy(g, j):
        return rcopy(pst.at[g, j], prx.at[g, 4 - j], ps.at[g, j], pr.at[g, 4 - j],
                     dev(x, (y + j) % 4, z, c))

    def tiles(count, which):
        def body(i, carry):
            g, j = which(i)

            def rows_body(b, inner):
                rows = pl.ds(pl.multiple_of(b * 256, 256), 256)
                part = jnp.dot(act[j, rows, :], wbuf[g], preferred_element_type=F32)
                pst[g, j, rows, :] = part.astype(BF)
                return inner

            lax.fori_loop(0, 2, rows_body, 0)

            @pl.when(j > 0)
            def _():
                p_copy(g, j).start()

            return carry

        lax.fori_loop(0, count, body, 0)

    def finish(g):
        for j in range(1, 4):
            recv(prx.at[g, j], pr.at[g, j])

        def body(b, carry):
            rows = pl.ds(pl.multiple_of(b * 128, 128), 128)
            total = pst[g, 0, rows, :].astype(F32) + bias[g]
            for j in range(1, 4):
                total = total + prx[g, j, rows, :].astype(F32)
            qkvs[g, rows, :] = total.astype(BF)
            return carry

        lax.fori_loop(0, 4, body, 0)

    slopes = slope_values(slope_index[...])

    def attend(h):
        def part(i, rows):
            b = h * 3 + i
            return qkvs[b // 2, rows, (b % 2) * HD:(b % 2 + 1) * HD]

        slope = slopes[h:h + 1, :]
        for i in range(4):
            rows = slice(i * 128, (i + 1) * 128)
            width = (i + 1) * 128
            upto = slice(0, width)
            scores = lax.dot_general(
                part(0, rows), part(1, upto), (((1,), (1,)), ((), ())),
                preferred_element_type=F32) / math.sqrt(HD)
            distance = (i * 128 + lax.broadcasted_iota(jnp.int32, (128, width), 0)
                        - lax.broadcasted_iota(jnp.int32, (128, width), 1)).astype(F32)
            scores = jnp.where(distance >= 0.0, scores - slope * distance, -1e30)
            highest = jnp.max(scores, axis=1, keepdims=True)
            powered = jnp.exp(scores - highest)
            attention = (powered / jnp.sum(powered, axis=1, keepdims=True)).astype(BF)
            context = jnp.dot(attention, part(2, upto), preferred_element_type=F32)
            cbuf[h, t, rows, :] = context.astype(BF)

    def source(q, cc):
        return ((xl + q // 4) % 2) * 8 + ((z + 4 - q % 4) % 4) * 2 + cc

    def c_copy(h, q):
        xx = x if q // 4 == 0 else x_in
        ref = cbuf.at[h, t]
        return rcopy(ref, ref, cs.at[h, q], cr.at[h, q], dev(xx, y, (z + q % 4) % 4, c))

    def f_copy(h, q):
        ref = cbuf.at[h, source(q, c)]
        return rcopy(ref, ref, fs.at[h, q], fr.at[h, q], other)

    def send_context(h):
        start([c_copy(h, q) for q in (1, 3, 4, 5, 7, 2, 6)])
        f_copy(h, 0).start()

    def relay_context(h):
        for q in (1, 3, 4, 5, 7, 2, 6):
            recv(cbuf.at[h, source(q, c)], cr.at[h, q])
            f_copy(h, q).start()

    def context_ready(h):
        for q in range(8):
            recv(cbuf.at[h, source(q, 1 - c)], fr.at[h, q])

    def project(h):
        def body(b, carry):
            rows = pl.ds(pl.multiple_of(b * 256, 256), 256)
            left = jnp.concatenate([cbuf[h, s, rows, :] for s in range(16)], axis=1)
            part = lax.dot_general(left, owr[h], (((1,), (1,)), ((), ())), preferred_element_type=F32)
            if h == 0:
                acc[rows, :] = part
            else:
                out[rows, :] = (acc[rows, :] + part + obias[...]).astype(BF)
            return carry

        lax.fori_loop(0, 2, body, 0)

    send_weights(0)
    lax.fori_loop(0, 2, norm_share, 0)
    relay_weight(2)
    o_load(0).start()
    o_load(1).start()
    for k in W_ORDER:
        w_arrive(0, k)
    lax.fori_loop(0, 2, norm_own, 0)
    y_arrive(1, 0)
    y_arrive(3, 0)
    send_weights(1)
    relay_out(0)
    relay_out(1)
    y_arrive(1, 1)
    y_arrive(3, 1)
    for p in range(2):
        pass
    w_ready(0)
    d_arrive(0)
    tiles(1, lambda i: (0, i))
    for k in W_ORDER[:3]:
        w_arrive(1, k)
    a_arrive(1, 0)
    a_arrive(3, 0)
    for k in W_ORDER[3:]:
        w_arrive(1, k)
    y_arrive(2, 0)
    send_weights(2)
    relay_out(2)
    relay_out(3)
    y_arrive(2, 1)
    a_arrive(1, 1)
    a_arrive(3, 1)
    d_arrive(1)
    d_arrive(3)
    tiles(2, lambda i: (0, 1 + 2 * i))
    w_arrive(2, W_ORDER[0])
    w_ready(1)
    tiles(3, lambda i: (1, (1 + 2 * i) % 5))
    for k in W_ORDER[1:]:
        w_arrive(2, k)
    relay_out(4)
    relay_out(5)
    a_arrive(2, 0)
    a_arrive(2, 1)
    d_arrive(2)
    tiles(2, lambda i: (i, 2))
    w_ready(2)
    tiles(2, lambda i: (2, 1 + 2 * i))
    tiles(2, lambda i: (2, 2 - 2 * i))
    relay_out(6)
    finish(0)
    finish(1)
    attend(0)
    send_context(0)
    finish(2)
    attend(1)
    send_context(1)
    relay_context(0)
    context_ready(0)
    project(0)
    relay_context(1)
    context_ready(1)
    project(1)

    for g in range(3):
        for k in range(8):
            if k:
                for cp in z_copies(g, k):
                    cp.wait_send()
            for cp in x_copies(g, k):
                cp.wait_send()
        for j in range(1, 4):
            p_copy(g, j).wait_send()
    for p in range(2):
        for d in range(1, 4):
            y_copy(p, d).wait_send()
            a_copy(d, p).wait_send()
        for j in range(4):
            for lvl in range(2):
                d_copy(j, p, lvl).wait_send()
    for h in range(2):
        for q in range(8):
            if q:
                c_copy(h, q).wait_send()
            f_copy(h, q).wait_send()


def shards(hidden, ln_gain, ln_shift, qkv_weight, qkv_bias, out_weight, out_bias, slope_index):
    dma = pltpu.SemaphoreType.DMA
    anyspec = pl.BlockSpec(memory_space=pl.ANY)
    vm = pl.BlockSpec(memory_space=pltpu.VMEM)
    return pl.pallas_call(
        kernel,
        out_shape=jax.ShapeDtypeStruct((SEQ, out_weight.shape[0]), BF),
        in_specs=[anyspec, anyspec, vm, vm, vm, anyspec, vm, vm],
        out_specs=vm,
        scratch_shapes=[
            pltpu.VMEM((WR, 32, 384), BF),
            pltpu.VMEM((3, 16, WR, GW), BF),
            pltpu.VMEM((2, 4, ROWS, KB), BF),
            pltpu.VMEM((2, 4, ROWS, KB), BF),
            pltpu.VMEM((4, SEQ, KB), BF),
            pltpu.VMEM((3, KB, GW), BF),
            pltpu.VMEM((3, 8, WR, GW), BF),
            pltpu.VMEM((3, 4, SEQ, GW), BF),
            pltpu.VMEM((3, 4, SEQ, GW), BF),
            pltpu.VMEM((3, SEQ, GW), BF),
            pltpu.VMEM((2, OC, 32, HD), BF),
            pltpu.VMEM((2, 896, 2048), BF),
            pltpu.VMEM((2, 16, SEQ, HD), BF),
            pltpu.VMEM((SEQ, 896), F32),
            dma((1,)), dma((2, 2, 4)), dma((7,)),
            dma((3, 8, 2)), dma((3, 8, 2)),
            dma((3, 4, 8)), dma((3, 4, 8)),
            dma((2, 4)), dma((2, 4)),
            dma((4, 2)), dma((4, 2)),
            dma((4, 2, 2)), dma((4, 2, 2)),
            dma((3, 4)), dma((3, 4)),
            dma((2, 8)), dma((2, 8)),
            dma((2, 8)), dma((2, 8)),
        ],
        compiler_params=pltpu.CompilerParams(
            collective_id=0, has_side_effects=True, vmem_limit_bytes=67043328),
        name="attention_block",
    )(
        qkv_weight,
        hidden,
        ln_gain.reshape(4, 1, KB),
        ln_shift.reshape(4, 1, KB),
        qkv_bias.reshape(3, 1, GW),
        out_weight,
        out_bias.reshape(1, -1),
        slope_index.reshape(2, 1),
    )


def solution(mesh):
    return jax.shard_map(
        shards,
        mesh=mesh,
        in_specs=(
            P("rep", None),
            P(),
            P(),
            P(("rep", "tp"), None, None),
            P("tp", None),
            P("tp", None, None),
            P("tp"),
            P("tp"),
        ),
        out_specs=P("rep", "tp"),
        check_vma=False,
    )
```

```python
import math

import jax
import jax.numpy as jnp
from jax import lax
from jax.experimental import pallas as pl
from jax.experimental.pallas import tpu as pltpu
from jax.sharding import PartitionSpec as P

N_SLOPES = 112
epsilon = 1e-05
MESH = pl.DeviceIdType.MESH
BF = jnp.bfloat16
F32 = jnp.float32

SEQ = 512
ROWS = 64
KB = 3584
WR = 112
GW = 256
HD = 128
OC = 128
W_ORDER = (1, 2, 6, 3, 7, 4, 5)


def slope_values(slope_index):
    power = 1 << N_SLOPES.bit_length() - 1
    index_float = slope_index.astype(jnp.float32)
    leading = jnp.exp2(-8.0 * (index_float + 1.0) / power)
    between = jnp.exp2(-4.0 * (2.0 * (index_float - power) + 1.0) / power)
    return jnp.where(slope_index < power, leading, between)


def dev(x, y, z, c):
    return (y * 2 + x // 2, (x % 2) * 8 + z * 2 + c)


def kernel(
    wq, hid, gain, shift, bias, ow, obias, slope_index, out,
    wsrc, wtv, hbuf, nrm, act, wbuf, stg, pst, prx, qkvs, owc, owr, cbuf, acc,
    wl, hs, ol, zs, zr, xs, xr, ys, yr, as_, ar, ds_, dr, ps, pr, cs, cr, fs, fr,
):
    r = lax.axis_index("rep")
    t = lax.axis_index("tp")
    y = r // 2
    xl = t // 8
    x = (r % 2) * 2 + xl
    z = (t // 2) % 4
    c = t % 2
    x_in = (x // 2) * 2 + (1 - xl)
    d_model = 4 * KB
    other = dev(x, y, z, 1 - c)

    bar = pltpu.get_barrier_semaphore()
    partners = []
    for k in range(1, 8):
        partners.append(dev(x, y, (z + k // 2) % 4, (c + k % 2) % 2))
    for d in range(1, 4):
        partners.append(dev((x + d) % 4, y, z, c))
        partners.append(dev(x, (y + d) % 4, z, c))
        partners.append(dev(x_in, y, (z + d) % 4, c))
    for p in partners:
        pl.semaphore_signal(bar, inc=1, device_id=p, device_id_type=MESH)

    def half(p):
        return (z + p) % 2

    def row_of(p, hf, cc):
        return pl.multiple_of(p * 256 + hf * 128 + cc * 64, 64)

    wload = pltpu.make_async_copy(wq, wsrc, wl.at[0])
    wload.start()

    def h_load(p, hf, lvl, b):
        return pltpu.make_async_copy(
            hid.at[pl.ds(row_of(p, hf, c), ROWS), pl.ds(b * KB, KB)], hbuf.at[p, b], hs.at[p, lvl, b])

    for p in range(2):
        for b in range(4):
            h_load(p, half(p), 0, b).start()

    def o_load(i):
        return pltpu.make_async_copy(ow.at[pl.ds(i * OC, OC)], owc.at[i % 2], ol.at[i])

    def relay_out(i):
        o_load(i).wait()

        def body(b, carry):
            rows = pl.ds(pl.multiple_of(b * 16, 16), 16)
            dst = pl.ds(pl.multiple_of(i * OC + b * 16, 16), 16)
            turned = jnp.swapaxes(owc[i % 2, rows], 0, 1)
            for h in range(32):
                owr[h % 2, dst, (h // 2) * HD:(h // 2 + 1) * HD] = turned[h]
            return carry

        lax.fori_loop(0, OC // 16, body, 0)
        if i + 2 < 7:
            o_load(i + 2).start()

    def relay_weight(col):
        def body(b, carry):
            rows = pl.ds(pl.multiple_of(b * 16, 16), 16)
            turned = jnp.swapaxes(wsrc[rows, :, col * HD:(col + 1) * HD], 0, 1)
            for h in range(32):
                blk = (h % 2) * 3 + col
                wtv[blk // 2, h // 2, rows, (blk % 2) * HD:(blk % 2 + 1) * HD] = turned[h]
            return carry

        lax.fori_loop(0, WR // 16, body, 0)

    wload.wait()
    relay_weight(0)
    relay_weight(1)
    pl.semaphore_wait(bar, len(partners))

    def rcopy(src, dst, ss, rs, to):
        return pltpu.make_async_remote_copy(
            src_ref=src, dst_ref=dst, send_sem=ss, recv_sem=rs, device_id=to, device_id_type=MESH)

    def recv(dst, rs):
        rcopy(dst, dst, zs.at[0, 0, 0], rs, other).wait_recv()

    def slot(xx, k):
        s = ((z + 4 - k // 2) % 4) * 2 + (c + k % 2) % 2
        return pl.ds(pl.multiple_of((xx * 8 + s) * WR, 16), WR)

    tp_own = xl * 8 + z * 2 + c
    tp_oth = (1 - xl) * 8 + z * 2 + c

    def z_copies(g, k):
        zz, cc = (z + k // 2) % 4, (c + k % 2) % 2
        to = dev(x, y, zz, cc)
        return (
            rcopy(wtv.at[g, xl * 8 + zz * 2 + cc], wbuf.at[g, slot(x, 0), :],
                  zs.at[g, k, 0], zr.at[g, k, 0], to),
            rcopy(wtv.at[g, (1 - xl) * 8 + zz * 2 + cc], stg.at[g, k],
                  zs.at[g, k, 1], zr.at[g, k, 1], to),
        )

    def x_copies(g, k):
        rows = slot(x, k)
        side = wtv.at[g, tp_oth] if k == 0 else stg.at[g, k]
        across = wtv.at[g, tp_own] if k == 0 else wbuf.at[g, rows, :]
        return [
            rcopy(src, wbuf.at[g, rows, :], xs.at[g, d, k], xr.at[g, d, k],
                  dev((x + d) % 4, y, z, c))
            for d, src in ((1, side), (3, side), (2, across))
        ]

    def start(copies):
        for cp in copies:
            cp.start()

    def send_weights(g):
        for k in W_ORDER:
            start(z_copies(g, k))
        start(x_copies(g, 0))
        wbuf[g, slot(x, 0), :] = wtv[g, tp_own]

    def w_arrive(g, k):
        recv(wbuf.at[g, slot(x, k), :], zr.at[g, k, 0])
        recv(stg.at[g, k], zr.at[g, k, 1])
        start(x_copies(g, k))

    def w_ready(g):
        for k in range(8):
            for d in range(1, 4):
                recv(wbuf.at[g, slot((x + 4 - d) % 4, k), :], xr.at[g, d, k])

    step = 512
    nblk = KB // step

    def stats(p, rows):
        total = jnp.zeros((16, step), F32)
        for i in range(4 * nblk):
            o = (i % nblk) * step
            total = total + hbuf[p, i // nblk, rows, o:o + step].astype(F32)
        mean = jnp.sum(total, axis=1, keepdims=True) / d_model
        total = jnp.zeros((16, step), F32)
        for i in range(4 * nblk):
            o = (i % nblk) * step
            centred = hbuf[p, i // nblk, rows, o:o + step].astype(F32) - mean
            total = total + centred * centred
        var = jnp.sum(total, axis=1, keepdims=True) / d_model
        return mean, lax.rsqrt(var + epsilon)

    def act_rows(j, p, hf, cc):
        return act.at[j, pl.ds(row_of(p, hf, cc), ROWS), :]

    def y_copy(p, d):
        return rcopy(nrm.at[p, (y + d) % 4], act_rows(4 - d, p, half(p), c),
                     ys.at[p, d], yr.at[p, 4 - d], dev(x, (y + d) % 4, z, c))

    def a_copy(j, p):
        ref = act_rows(j, p, half(p), c)
        to = dev(x, y, (z + 5 - 2 * half(p)) % 4, c)
        return rcopy(ref, ref, as_.at[j, p], ar.at[j, p], to)

    def d_copy(j, p, lvl):
        hf = half(p) if lvl == 0 else 1 - half(p)
        ref = act_rows(j, p, hf, c)
        return rcopy(ref, ref, ds_.at[j, p, lvl], dr.at[j, p, lvl], other)

    def norm_share(p, carry):
        for b in range(4):
            h_load(p, half(p), 0, b).wait()

        def body(rb, inner):
            rows = pl.ds(pl.multiple_of(rb * 16, 16), 16)
            mean, rstd = stats(p, rows)
            for i in range(4 * nblk):
                o = (i % nblk) * step
                centred = hbuf[p, i // nblk, rows, o:o + step].astype(F32) - mean
                val = centred * rstd * gain[i // nblk, :, o:o + step] + shift[i // nblk, :, o:o + step]
                nrm[p, i // nblk, rows, o:o + step] = val.astype(BF)
            return inner

        lax.fori_loop(0, ROWS // 16, body, 0)
        for b in range(4):
            h_load(p, 1 - half(p), 1, b).start()
        @pl.when(p == 0)
        def _():
            y_copy(0, 1).start()

        @pl.when(p == 1)
        def _():
            start([y_copy(1, 3), y_copy(1, 1), y_copy(0, 3), y_copy(0, 2), y_copy(1, 2)])

        act[0, pl.ds(row_of(p, half(p), c), ROWS), :] = nrm[p, y]
        d_copy(0, p, 0).start()
        return carry

    def norm_own(p, carry):
        for b in range(4):
            h_load(p, 1 - half(p), 1, b).wait()

        def body(rb, inner):
            rows = pl.ds(pl.multiple_of(rb * 16, 16), 16)
            mean, rstd = stats(p, rows)
            dst = pl.ds(pl.multiple_of(row_of(p, 1 - half(p), c) + rb * 16, 16), 16)
            for i in range(nblk):
                cols = slice(i * step, (i + 1) * step)
                centred = hbuf[p, y, rows, cols].astype(F32) - mean
                val = centred * rstd * gain[y, :, cols] + shift[y, :, cols]
                act[0, dst, cols] = val.astype(BF)
            return inner

        lax.fori_loop(0, ROWS // 16, body, 0)
        d_copy(0, p, 1).start()
        return carry

    def y_arrive(j, p):
        recv(act_rows(j, p, half(p), c), yr.at[p, j])
        start([a_copy(j, p), d_copy(j, p, 0)])

    def a_arrive(j, p):
        recv(act_rows(j, p, 1 - half(p), c), ar.at[j, p])
        d_copy(j, p, 1).start()

    def d_arrive(j):
        for p in range(2):
            for lvl in range(2):
                hf = half(p) if lvl == 0 else 1 - half(p)
                recv(act_rows(j, p, hf, 1 - c), dr.at[j, p, lvl])

    def p_copy(g, j, b):
        rows = pl.ds(pl.multiple_of(b * 256, 256), 256)
        return rcopy(pst.at[g, j, rows, :], prx.at[g, 4 - j, rows, :], ps.at[g, j, b], pr.at[g, 4 - j, b],
                     dev(x, (y + j) % 4, z, c))

    def tiles(count, which):
        def body(i, carry):
            g, j, b = which(i)
            rows = pl.ds(pl.multiple_of(b * 256, 256), 256)
            part = jnp.dot(act[j, rows, :], wbuf[g], preferred_element_type=F32)
            pst[g, j, rows, :] = part.astype(BF)

            @pl.when(j > 0)
            def _():
                p_copy(g, j, b).start()

            return carry

        lax.fori_loop(0, count, body, 0)

    def group_bias(g):
        parts = [bias[b // 3:b // 3 + 1, (b % 3) * HD:(b % 3 + 1) * HD] for b in (2 * g, 2 * g + 1)]
        return jnp.concatenate(parts, axis=1)

    def finish(g, b):
        rows = pl.ds(b * 256, 256)
        for j in range(1, 4):
            recv(prx.at[g, j, rows, :], pr.at[g, j, b])

        def body(i, carry):
            part = pl.ds(pl.multiple_of(b * 256 + i * 128, 128), 128)
            total = pst[g, 0, part, :].astype(F32) + group_bias(g)
            for j in range(1, 4):
                total = total + prx[g, j, part, :].astype(F32)
            qkvs[g, part, :] = total.astype(BF)
            return carry

        lax.fori_loop(0, 2, body, 0)

    def attend(h, b):
        def part(i, rows):
            n = h * 3 + i
            return qkvs[n // 2, rows, (n % 2) * HD:(n % 2 + 1) * HD]

        slope = slope_values(jnp.full((1, 1), slope_index[h], jnp.int32))
        for i in (2 * b, 2 * b + 1):
            rows = slice(i * 128, (i + 1) * 128)
            width = (i + 1) * 128
            upto = slice(0, width)
            scores = lax.dot_general(
                part(0, rows), part(1, upto), (((1,), (1,)), ((), ())),
                preferred_element_type=F32) / math.sqrt(HD)
            distance = (i * 128 + lax.broadcasted_iota(jnp.int32, (128, width), 0)
                        - lax.broadcasted_iota(jnp.int32, (128, width), 1)).astype(F32)
            scores = jnp.where(distance >= 0.0, scores - slope * distance, -1e30)
            highest = jnp.max(scores, axis=1, keepdims=True)
            powered = jnp.exp(scores - highest)
            attention = (powered / jnp.sum(powered, axis=1, keepdims=True)).astype(BF)
            context = jnp.dot(attention, part(2, upto), preferred_element_type=F32)
            cbuf[h, t, rows, :] = context.astype(BF)

    def source(q, cc):
        return ((xl + q // 4) % 2) * 8 + ((z + 4 - q % 4) % 4) * 2 + cc

    def c_copy(h, b, q):
        xx = x if q // 4 == 0 else x_in
        ref = cbuf.at[h, t, pl.ds(b * 256, 256), :]
        return rcopy(ref, ref, cs.at[h, b, q], cr.at[h, b, q], dev(xx, y, (z + q % 4) % 4, c))

    def f_copy(h, b, q):
        ref = cbuf.at[h, source(q, c), pl.ds(b * 256, 256), :]
        return rcopy(ref, ref, fs.at[h, b, q], fr.at[h, b, q], other)

    C_ORDER = (1, 3, 4, 5, 7, 2, 6)

    def send_context(h, b):
        start([c_copy(h, b, q) for q in C_ORDER])
        f_copy(h, b, 0).start()

    def relay_context(h, b):
        for q in C_ORDER:
            recv(cbuf.at[h, source(q, c), pl.ds(b * 256, 256), :], cr.at[h, b, q])
            f_copy(h, b, q).start()

    def context_ready(h, b):
        for q in range(8):
            recv(cbuf.at[h, source(q, 1 - c), pl.ds(b * 256, 256), :], fr.at[h, b, q])

    def project(h, b):
        rows = pl.ds(b * 256, 256)
        left = jnp.concatenate([cbuf[h, s, rows, :] for s in range(16)], axis=1)
        part = lax.dot_general(left, owr[h], (((1,), (1,)), ((), ())), preferred_element_type=F32)
        if h == 0:
            acc[rows, :] = part
        else:
            out[rows, :] = (acc[rows, :] + part + obias[...].reshape(1, 896)).astype(BF)

    send_weights(0)
    relay_weight(2)
    send_weights(1)
    lax.fori_loop(0, 2, norm_share, 0)
    o_load(0).start()
    o_load(1).start()
    for k in W_ORDER:
        w_arrive(0, k)
    lax.fori_loop(0, 2, norm_own, 0)
    y_arrive(1, 1)
    y_arrive(3, 0)
    relay_out(0)
    relay_out(1)
    for k in W_ORDER:
        w_arrive(1, k)
    y_arrive(1, 0)
    y_arrive(3, 1)
    send_weights(2)
    for i in range(2, 7):
        relay_out(i)
    w_ready(0)
    d_arrive(0)
    tiles(2, lambda i: (0, 0, i))
    a_arrive(1, 0)
    a_arrive(3, 1)
    y_arrive(2, 0)
    a_arrive(1, 1)
    a_arrive(3, 0)
    d_arrive(1)
    d_arrive(3)
    tiles(4, lambda i: (0, 1 + 2 * (i // 2), i % 2))
    y_arrive(2, 1)
    for k in W_ORDER:
        w_arrive(2, k)
    w_ready(1)
    tiles(6, lambda i: (1, (1 + 2 * (i // 2)) % 5, i % 2))
    a_arrive(2, 0)
    a_arrive(2, 1)
    d_arrive(2)
    tiles(4, lambda i: (i // 2, 2, i % 2))
    w_ready(2)
    tiles(8, lambda i: (2, (1 + 2 * (i % 4) + (i % 4) // 2) % 4, i // 4))
    for b in range(2):
        finish(0, b)
        finish(1, b)
        attend(0, b)
        send_context(0, b)
    finish(2, 0)
    attend(1, 0)
    send_context(1, 0)
    for b in range(2):
        relay_context(0, b)
    finish(2, 1)
    attend(1, 1)
    send_context(1, 1)
    for b in range(2):
        context_ready(0, b)
        project(0, b)
    for b in range(2):
        relay_context(1, b)
        context_ready(1, b)
        project(1, b)

    for g in range(3):
        for k in range(8):
            if k:
                for cp in z_copies(g, k):
                    cp.wait_send()
            for cp in x_copies(g, k):
                cp.wait_send()
        for j in range(1, 4):
            for b in range(2):
                p_copy(g, j, b).wait_send()
    for p in range(2):
        for d in range(1, 4):
            y_copy(p, d).wait_send()
            a_copy(d, p).wait_send()
        for j in range(4):
            for lvl in range(2):
                d_copy(j, p, lvl).wait_send()
    for h in range(2):
        for b in range(2):
            for q in range(8):
                if q:
                    c_copy(h, b, q).wait_send()
                f_copy(h, b, q).wait_send()


def shards(hidden, ln_gain, ln_shift, qkv_weight, qkv_bias, out_weight, out_bias, slope_index):
    dma = pltpu.SemaphoreType.DMA
    anyspec = pl.BlockSpec(memory_space=pl.ANY)
    vm = pl.BlockSpec(memory_space=pltpu.VMEM)
    return pl.pallas_call(
        kernel,
        out_shape=jax.ShapeDtypeStruct((SEQ, out_weight.shape[0]), BF),
        in_specs=[anyspec, anyspec, vm, vm, vm, anyspec, vm, pl.BlockSpec(memory_space=pltpu.SMEM)],
        out_specs=vm,
        scratch_shapes=[
            pltpu.VMEM((WR, 32, 384), BF),
            pltpu.VMEM((3, 16, WR, GW), BF),
            pltpu.VMEM((2, 4, ROWS, KB), BF),
            pltpu.VMEM((2, 4, ROWS, KB), BF),
            pltpu.VMEM((4, SEQ, KB), BF),
            pltpu.VMEM((3, KB, GW), BF),
            pltpu.VMEM((3, 8, WR, GW), BF),
            pltpu.VMEM((3, 4, SEQ, GW), BF),
            pltpu.VMEM((3, 4, SEQ, GW), BF),
            pltpu.VMEM((3, SEQ, GW), BF),
            pltpu.VMEM((2, OC, 32, HD), BF),
            pltpu.VMEM((2, 896, 2048), BF),
            pltpu.VMEM((2, 16, SEQ, HD), BF),
            pltpu.VMEM((SEQ, 896), F32),
            dma((1,)), dma((2, 2, 4)), dma((7,)),
            dma((3, 8, 2)), dma((3, 8, 2)),
            dma((3, 4, 8)), dma((3, 4, 8)),
            dma((2, 4)), dma((2, 4)),
            dma((4, 2)), dma((4, 2)),
            dma((4, 2, 2)), dma((4, 2, 2)),
            dma((3, 4, 2)), dma((3, 4, 2)),
            dma((2, 2, 8)), dma((2, 2, 8)),
            dma((2, 2, 8)), dma((2, 2, 8)),
        ],
        compiler_params=pltpu.CompilerParams(
            collective_id=0, has_side_effects=True, vmem_limit_bytes=67043328),
        name="attention_block",
    )(
        qkv_weight,
        hidden,
        ln_gain.reshape(4, 1, KB),
        ln_shift.reshape(4, 1, KB),
        qkv_bias,
        out_weight,
        out_bias,
        slope_index,
    )


def solution(mesh):
    return jax.shard_map(
        shards,
        mesh=mesh,
        in_specs=(
            P("rep", None),
            P(),
            P(),
            P(("rep", "tp"), None, None),
            P("tp", None),
            P("tp", None, None),
            P("tp"),
            P("tp"),
        ),
        out_specs=P("rep", "tp"),
        check_vma=False,
    )
```
